128 devices in a mesh: samp: 64 (over x, y, z), tp: 2 (over core).
Axes of the slice: x: 4, y: 4, z: 4, core: 2. Of those that a mesh axis runs over, the one named last changes fastest.
Arguments:
- images: bfloat16 [128, 12288], P(None, 'tp'), may hold values from -6 to 6
- enc_mean: float32 [128, 128], replicated, may hold values from -0.3 to 0.3
- enc_logscale: float32 [128, 128], replicated, may hold values from -0.15 to 0
- noise: float32 [128, 512, 128], P(None, 'samp'), may hold values from -5 to 5
- w_in: bfloat16 [128, 1024], P(None, 'tp'), may hold values from -0.5 to 0.5
- b_in: bfloat16 [1, 1024], P(None, 'tp'), may hold values from -3 to 3
- w_out: bfloat16 [1024, 12288], P(None, 'tp'), may hold values from -0.0078125 to 0.0078125
- b_out: float32 [1, 12288], P(None, 'tp'), may hold values from -3 to 3
- pixel_logscale: float32 [1, 12288], P(None, 'tp'), may hold values from 0 to 1
Outputs:
- bound: float32 [128], replicated
- log_weights: float32 [128, 512], P(None, 'samp')
The draws below stay inside these ranges and needn't reach their ends.
All inputs are finite; a program needn't handle non-finite values.
Results may differ from the reference program's by a relative error of at most 0.00073.
Values may be sent and summed in bfloat16 or wider, within the bound.
A program may use at most 64 MiB of HBM per device.

```python
import math
import jax
import jax.numpy as jnp
from jax import lax

PIX = 12288
HID = 1024
LAT = 128
IMG = 128
K = 512


def draw_w_out(key, part):
    dense_key = jax.random.fold_in(key, 101)
    row_key = jax.random.fold_in(key, 202)
    column_key = jax.random.fold_in(key, 303)
    deviation = 2.5 / math.sqrt(HID * 2048)
    dense_part = jax.random.normal(dense_key, (HID, PIX), jnp.float32) * deviation
    row_factor = jax.random.normal(row_key, (HID,), jnp.float32)
    column_factor = jax.random.normal(column_key, (PIX,), jnp.float32)
    combined = dense_part + 0.5 * deviation * row_factor[:, None] * column_factor[None, :]
    return jnp.clip(combined, -0.0078125, 0.0078125).astype(jnp.bfloat16)


def block_scale(key, dims, split, least, top_value):
    def one(axis_at, shards_of):
        heights = jax.random.uniform(jax.random.fold_in(jax.random.fold_in(key, 6), axis_at), (shards_of,), jnp.float32, least / len(split), top_value / len(split))
        return jnp.repeat(jnp.exp(heights), dims[axis_at] // shards_of).reshape((-1,) + (1,) * (len(dims) - axis_at - 1))

    level = one(*split[0])
    for cut in split[1:]:
        level = level * one(*cut)
    return level


def gaussian(own_key, extent, spread, reach, split=(), held_as=jnp.bfloat16):
    level = block_scale(own_key, extent, split, -0.22, 0.18) if split else 1.0
    result = jax.random.normal(own_key, extent, jnp.float32) * spread * level
    return jnp.minimum(jnp.maximum(result, -reach), reach).astype(held_as)


def setup_inputs(seed: int = 0) -> dict:
    keys = jax.random.split(jax.random.key(seed), 10)
    return {
        "images": gaussian(keys[0], (IMG, PIX), 1.0, 6.0, ((1, 2),)),
        "enc_mean": gaussian(keys[1], (IMG, LAT), 0.05, 0.3, (), jnp.float32),
        "enc_logscale": jnp.clip(jax.random.uniform(keys[2], (IMG, LAT), jnp.float32, -0.15, 0.0), -0.15, 0.0),
        "noise": gaussian(keys[3], (IMG, K, LAT), 1.0, 5.0, ((1, 64),), jnp.float32),
        "w_in": gaussian(keys[4], (LAT, HID), LAT ** -0.5, 0.5, ((1, 2),)),
        "b_in": gaussian(keys[5], (1, HID), 0.5, 3.0, ((1, 2),)),
        "w_out": draw_w_out(jax.random.fold_in(keys[9], 71), 0),
        "b_out": gaussian(keys[7], (1, PIX), 0.5, 3.0, ((1, 2),), jnp.float32),
        "pixel_logscale": jnp.clip(1.0 * jax.random.uniform(keys[8], (1, PIX), jnp.float32) ** block_scale(keys[8], (1, PIX), ((1, 2),), -0.2, 0.2), 0.0, 1.0),
    }


HALF_LOG_TAU = 0.9189385332046727


def reference(images, enc_mean, enc_logscale, noise, w_in, b_in, w_out, b_out, pixel_logscale):
    latent = enc_mean[:, None, :] + jnp.exp(enc_logscale)[:, None, :] * noise
    inverse = jnp.exp(-pixel_logscale)
    constant = -jnp.sum(pixel_logscale) - PIX * HALF_LOG_TAU

    def image_loglik(operands):
        latent_one, image_one = operands
        latent_rows = latent_one.astype(jnp.bfloat16)
        hidden = jax.nn.relu(jnp.dot(latent_rows, w_in, preferred_element_type=jnp.float32) + b_in.astype(jnp.float32)).astype(jnp.bfloat16)
        pixel_mean = jnp.dot(hidden, w_out, preferred_element_type=jnp.float32) + b_out
        scaled = (image_one[None, :].astype(jnp.float32) - pixel_mean) * inverse
        return jnp.sum(-0.5 * scaled * scaled, axis=1)

    loglik = lax.map(image_loglik, (latent, images)) + constant
    prior = jnp.sum(-0.5 * latent * latent - HALF_LOG_TAU, axis=2)
    posterior = jnp.sum(-0.5 * noise * noise - enc_logscale[:, None, :] - HALF_LOG_TAU, axis=2)
    logw = loglik + prior - posterior
    peak = jnp.max(logw, axis=1)
    sum_exp = jnp.sum(jnp.exp(logw - peak[:, None]), axis=1)
    bound = (peak + jnp.log(sum_exp) - jnp.log(jnp.float32(K))) / PIX
    log_weights = (logw - peak[:, None]) - jnp.log(sum_exp)[:, None] + jnp.log(jnp.float32(K))
    return bound, log_weights
```

```python
import functools
import math

import jax
import jax.numpy as jnp
from jax import lax
from jax.experimental import pallas as pl
from jax.experimental.pallas import tpu as pltpu
from jax.sharding import PartitionSpec as P

HALF_LOG_TAU = 0.9189385332046727
MESH = pl.DeviceIdType.MESH
F32 = jnp.float32
BF16 = jnp.bfloat16
NT = (((1,), (1,)), ((), ()))
G_ROWS = ((0, 48), (48, 48), (96, 48), (144, 48), (192, 32), (224, 32))
C_ROWS = ((0, 88), (88, 88), (176, 88), (264, 88), (352, 80), (432, 80))
SIDE = 4


def kernel(
    images, enc_mean, enc_ls, noise, w_in, b_in, w_out, b_out, pls,
    bound_ref, lw_ref,
    wv, ws, img, dv, bv, pv, nz, em, el, wbuf, bbuf, wat, lat, hid, gbuf, cbuf,
    s2v, acc_sq, pp, lsend, lrecv, sbuf, rbuf,
    in_sem, g_send, g_recv, pair_send, pair_recv, x_send, x_recv,
):
    me = lax.axis_index("samp")
    t = lax.axis_index("tp")
    x, y, z = me // (SIDE * SIDE), (me // SIDE) % SIDE, me % SIDE
    color = (x + y + z) % 2
    pixels = img.shape[1]
    all_pixels = 2 * pixels
    all_samples = 8 * SIDE * SIDE * SIDE

    def at(xx, yy, zz):
        return (xx % SIDE) * (SIDE * SIDE) + (yy % SIDE) * SIDE + zz % SIDE

    line = {
        "z": [at(x, y, z + k) for k in (1, 2, 3)],
        "y": [at(x, y + k, z) for k in (1, 2, 3)],
        "x": [at(x + k, y, z) for k in (1, 2, 3)],
    }
    near = [
        at(x + 1, y, z), at(x + 3, y, z), at(x, y + 1, z),
        at(x, y + 3, z), at(x, y, z + 1), at(x, y, z + 3),
    ]

    barrier = pltpu.get_barrier_semaphore()
    pl.semaphore_signal(barrier, inc=1, device_id=(me, 1 - t), device_id_type=MESH)
    for axis in ("x", "y", "z"):
        for other in line[axis]:
            pl.semaphore_signal(barrier, inc=1, device_id=(other, t), device_id_type=MESH)

    def slabs(p):
        return 2 * p, 2 * p + 1, 2 - p, 3 - 3 * p

    own = slabs(color)
    height = wv.shape[1]

    def load(src, dst, k):
        return pltpu.make_async_copy(src, dst, in_sem.at[k])

    loads = [
        load(noise, nz, 0), load(enc_mean, em, 1), load(enc_ls, el, 2),
        load(w_in, wbuf.at[t], 3), load(b_in, bbuf.at[t], 4),
        load(pls, pv, 5), load(b_out, bv, 6),
    ]
    slab = [
        load(w_out.at[pl.ds(pl.multiple_of(own[k] * height, height), height), :], wv.at[k], 7 + k)
        for k in range(4)
    ]
    load_img = load(images, img, 11)
    for c in loads:
        c.start()
    slab[0].start()
    load_img.start()
    for k in (1, 2, 3):
        slab[k].start()

    for k in (0, 1, 2):
        loads[k].wait()
    mean_t = em[...].T
    ls_t = el[...].T
    exp_t = jnp.exp(ls_t)
    ls_sum = jnp.sum(ls_t, axis=0, keepdims=True)
    for s in range(8):
        n_t = nz[pl.ds(s, 128, stride=8), :].T
        l_t = mean_t + exp_t * n_t
        lat[0:128, s * 128 : (s + 1) * 128] = l_t.astype(BF16)
        pp[s : s + 1, :] = 0.5 * jnp.sum(n_t * n_t - l_t * l_t, axis=0, keepdims=True) + ls_sum
    first_row = lax.broadcasted_iota(jnp.int32, (128, 1024), 0) == 0
    lat[128:256, :] = jnp.where(first_row, 1.0, 0.0).astype(BF16)

    loads[5].wait()
    loads[6].wait()
    s2v[...] = jnp.exp(-2.0 * pv[...])
    total_ls = jnp.sum(pv[...], axis=1, keepdims=True)

    def scale(k):
        for c in range(pixels // 256):
            cols = slice(c * 256, (c + 1) * 256)
            factor = s2v[:, cols].astype(BF16)
            ws[k, :, cols] = wv[k, :, cols] * factor

    def gram(k, j):
        return lax.dot_general(ws[k], wv[j], NT, preferred_element_type=F32)

    def sends(q):
        out = []
        for d in range(6):
            lo, n = G_ROWS[d] if q < 5 else C_ROWS[d]
            ref = gbuf.at[color, q, pl.ds(lo, n), :] if q < 5 else cbuf.at[color, pl.ds(lo, n), :]
            out.append(
                pltpu.make_async_remote_copy(
                    src_ref=ref, dst_ref=ref, send_sem=g_send.at[q, d], recv_sem=g_recv.at[q, d],
                    device_id=(near[d], t), device_id_type=MESH,
                )
            )
        return out

    def receives(q):
        out = []
        for d in range(6):
            lo, n = G_ROWS[d] if q < 5 else C_ROWS[d]
            c = 1 - color
            ref = gbuf.at[c, q, pl.ds(lo, n), :] if q < 5 else cbuf.at[c, pl.ds(lo, n), :]
            out.append(
                pltpu.make_async_remote_copy(
                    src_ref=ref, dst_ref=ref, send_sem=g_send.at[q, d], recv_sem=g_recv.at[q, d],
                    device_id=(near[d], t), device_id_type=MESH,
                )
            )
        return out

    all_sends = [sends(q) for q in range(6)]

    slab[0].wait()
    scale(0)
    load_img.wait()
    acc_sq[...] = jnp.zeros_like(acc_sq)
    gbuf[color, 0] = (0.5 * gram(0, 0)).astype(BF16)
    for c in range(pixels // 256):
        cols = slice(c * 256, (c + 1) * 256)
        d = img[:, cols].astype(F32) - bv[:, cols]
        e = d * s2v[:, cols]
        hi = e.astype(BF16)
        dv[0:128, cols] = hi
        dv[128:256, cols] = (e - hi.astype(F32)).astype(BF16)
        sq = d * e
        acc_sq[...] += sq[:, 0:128] + sq[:, 128:256]

    loads[3].wait()
    loads[4].wait()
    pl.semaphore_wait(barrier, 10)
    weights = pltpu.make_async_remote_copy(
        src_ref=wbuf.at[t], dst_ref=wbuf.at[t], send_sem=pair_send.at[0], recv_sem=pair_recv.at[0],
        device_id=(me, 1 - t), device_id_type=MESH,
    )
    biases = pltpu.make_async_remote_copy(
        src_ref=bbuf.at[t], dst_ref=bbuf.at[t], send_sem=pair_send.at[1], recv_sem=pair_recv.at[1],
        device_id=(me, 1 - t), device_id_type=MESH,
    )
    weights.start()
    biases.start()
    for c in all_sends[0]:
        c.start()

    slab[1].wait()
    scale(1)
    gbuf[color, 1] = gram(0, 1).astype(BF16)
    for c in all_sends[1]:
        c.start()
    gbuf[color, 2] = (0.5 * gram(1, 1)).astype(BF16)
    for c in all_sends[2]:
        c.start()
    for k in range(2):
        both = lax.dot_general(wv[k], dv[...], NT, preferred_element_type=F32)
        cbuf[color, k * 256 : (k + 1) * 256, :] = both[:, 0:128] + both[:, 128:256]
    for c in all_sends[5]:
        c.start()
    slab[2].wait()
    gbuf[color, 3] = gram(0, 2).astype(BF16)
    for c in all_sends[3]:
        c.start()
    slab[3].wait()
    gbuf[color, 4] = gram(1, 3).astype(BF16)
    for c in all_sends[4]:
        c.start()

    theirs_w = pltpu.make_async_remote_copy(
        src_ref=wbuf.at[1 - t], dst_ref=wbuf.at[1 - t], send_sem=pair_send.at[0], recv_sem=pair_recv.at[0],
        device_id=(me, 1 - t), device_id_type=MESH,
    )
    theirs_b = pltpu.make_async_remote_copy(
        src_ref=bbuf.at[1 - t], dst_ref=bbuf.at[1 - t], send_sem=pair_send.at[1], recv_sem=pair_recv.at[1],
        device_id=(me, 1 - t), device_id_type=MESH,
    )
    theirs_w.wait_recv()
    theirs_b.wait_recv()
    for k in range(2):
        row0 = lax.broadcasted_iota(jnp.int32, (128, 512), 0) == 0
        bias = jnp.where(row0, bbuf[k].astype(F32), 0.0)
        wat[k * 512 : (k + 1) * 512, 0:128] = wbuf[k].astype(F32).T.astype(BF16)
        wat[k * 512 : (k + 1) * 512, 128:256] = bias.T.astype(BF16)
    for k in range(4):
        rows = slice(k * 256, (k + 1) * 256)
        pre = jnp.dot(wat[rows, :], lat[...], preferred_element_type=F32)
        hid[k] = jnp.maximum(pre, 0.0).astype(BF16)

    def apply(p, which):
        o1, o2, x1, x2 = slabs(p)
        for n in range(4):
            cols = slice(n * 256, (n + 1) * 256)
            y1 = jnp.dot(gbuf[p, 0], hid[o1, :, cols], preferred_element_type=F32)
            y1 += jnp.dot(gbuf[p, 1], hid[o2, :, cols], preferred_element_type=F32)
            y1 += jnp.dot(gbuf[p, 3], hid[x1, :, cols], preferred_element_type=F32)
            y2 = jnp.dot(gbuf[p, 2], hid[o2, :, cols], preferred_element_type=F32)
            y2 += jnp.dot(gbuf[p, 4], hid[x2, :, cols], preferred_element_type=F32)
            for h in range(2):
                s = 2 * n + h
                part = slice(h * 128, (h + 1) * 128)
                lanes = slice(s * 128, (s + 1) * 128)
                total = jnp.sum(
                    (cbuf[p, 0:256, :] - y1[:, part]) * hid[o1, :, lanes].astype(F32)
                    + (cbuf[p, 256:512, :] - y2[:, part]) * hid[o2, :, lanes].astype(F32),
                    axis=0, keepdims=True,
                )
                if which == 0:
                    lsend[s : s + 1, :] = total
                else:
                    lsend[s : s + 1, :] += total

    apply(color, 0)
    image_part = -0.5 * jnp.sum(acc_sq[...].T, axis=0, keepdims=True)
    lsend[8:16, :] = jnp.broadcast_to(image_part - total_ls - pixels * HALF_LOG_TAU, (8, 128))
    for q in (0, 1, 2, 5, 3, 4):
        for c in receives(q):
            c.wait_recv()
    apply(1 - color, 1)

    share = pltpu.make_async_remote_copy(
        src_ref=lsend, dst_ref=lrecv, send_sem=pair_send.at[2], recv_sem=pair_recv.at[2],
        device_id=(me, 1 - t), device_id_type=MESH,
    )
    share.start()
    share.wait_recv()
    loglik = lsend[...] + lrecv[...]
    image_term = loglik[8:9, :]
    logw = loglik[0:8, :] + pp[...]
    peak = jnp.max(logw, axis=0, keepdims=True)
    sums = jnp.sum(jnp.exp(logw - peak), axis=0, keepdims=True)
    rounds = []
    for r, axis in enumerate(("z", "y", "x")):
        sbuf[r, 0:1, :] = peak
        sbuf[r, 1:2, :] = sums
        copies = [
            pltpu.make_async_remote_copy(
                src_ref=sbuf.at[r], dst_ref=rbuf.at[r, k], send_sem=x_send.at[r, k],
                recv_sem=x_recv.at[r, k], device_id=(line[axis][k], t), device_id_type=MESH,
            )
            for k in range(3)
        ]
        for c in copies:
            c.start()
        for c in copies:
            c.wait_recv()
        rounds += copies
        top = peak
        for k in range(3):
            top = jnp.maximum(top, rbuf[r, k, 0:1, :])
        sums = sums * jnp.exp(peak - top)
        for k in range(3):
            sums += rbuf[r, k, 1:2, :] * jnp.exp(rbuf[r, k, 0:1, :] - top)
        peak = top
    log_sum = jnp.log(sums)
    log_all = math.log(all_samples)
    bound_ref[...] = (image_term + peak + log_sum - log_all) / all_pixels
    lw_ref[...] = logw - peak - log_sum + log_all

    for c in rounds + [share, weights, biases]:
        c.wait_send()
    for q in range(6):
        for c in all_sends[q]:
            c.wait_send()


def on_device(images, enc_mean, enc_logscale, noise, w_in, b_in, w_out, b_out, pixel_logscale):
    image_count, sample_count, latent_dims = noise.shape
    hidden, pixels = w_out.shape
    height = hidden // 4
    noise = noise.reshape(image_count * sample_count, latent_dims)
    half = w_in.shape[1]
    V = pltpu.VMEM
    bound, lw = pl.pallas_call(
        kernel,
        out_shape=(
            jax.ShapeDtypeStruct((1, image_count), F32),
            jax.ShapeDtypeStruct((sample_count, image_count), F32),
        ),
        in_specs=[pl.BlockSpec(memory_space=pl.ANY)] * 9,
        out_specs=[pl.BlockSpec(memory_space=pltpu.VMEM)] * 2,
        scratch_shapes=[
            V((4, height, pixels), BF16), V((2, height, pixels), BF16), V((image_count, pixels), BF16),
            V((2 * image_count, pixels), BF16), V((1, pixels), F32), V((1, pixels), F32),
            V(noise.shape, F32), V((image_count, latent_dims), F32), V((image_count, latent_dims), F32),
            V((2, latent_dims, half), BF16), V((2, 1, half), BF16), V((hidden, 256), BF16),
            V((256, image_count * sample_count), BF16), V((4, height, image_count * sample_count), BF16),
            V((2, 5, height, height), BF16), V((2, 2 * height, image_count), F32),
            V((1, pixels), F32), V((image_count, 128), F32), V((sample_count, image_count), F32),
            V((16, image_count), F32), V((16, image_count), F32),
            V((3, 8, image_count), F32), V((3, 3, 8, image_count), F32),
            pltpu.SemaphoreType.DMA((12,)), pltpu.SemaphoreType.DMA((6, 6)), pltpu.SemaphoreType.DMA((6, 6)),
            pltpu.SemaphoreType.DMA((3,)), pltpu.SemaphoreType.DMA((3,)),
            pltpu.SemaphoreType.DMA((3, 3)), pltpu.SemaphoreType.DMA((3, 3)),
        ],
        compiler_params=pltpu.CompilerParams(
            collective_id=0, has_side_effects=True, vmem_limit_bytes=60 * 1024 * 1024
        ),
    )(images, enc_mean, enc_logscale, noise, w_in, b_in, w_out, b_out, pixel_logscale)
    return bound.reshape(image_count), lw.T


def solution(mesh):
    pixel_split = P(None, "tp")
    in_specs = (
        pixel_split, P(), P(), P(None, "samp", None),
        pixel_split, pixel_split, pixel_split, pixel_split, pixel_split,
    )
    out_specs = (P(), P(None, "samp"))
    return jax.shard_map(
        on_device, mesh=mesh, in_specs=in_specs, out_specs=out_specs, check_vma=False
    )
```

```python
import functools
import math

import jax
import jax.numpy as jnp
from jax import lax
from jax.experimental import pallas as pl
from jax.experimental.pallas import tpu as pltpu
from jax.sharding import PartitionSpec as P

HALF_LOG_TAU = 0.9189385332046727
MESH = pl.DeviceIdType.MESH
F32 = jnp.float32
BF16 = jnp.bfloat16
NT = (((1,), (1,)), ((), ()))
G_ROWS = ((0, 48), (48, 48), (96, 48), (144, 48), (192, 32), (224, 32))
C_ROWS = ((0, 88), (88, 88), (176, 88), (264, 88), (352, 80), (432, 80))
SIDE = 4


def kernel(
    images, enc_mean, enc_ls, noise, w_in, b_in, w_out, b_out, pls,
    bound_ref, lw_ref,
    wv, ws, img, dv, bv, pv, nz, em, el, wbuf, bbuf, wat, lat, hid, gbuf, cbuf,
    g_half, s2v, acc_sq, pp, lsend, lrecv, sbuf, rbuf,
    in_sem, g_send, g_recv, pair_send, pair_recv, x_send, x_recv,
):
    me = lax.axis_index("samp")
    t = lax.axis_index("tp")
    x, y, z = me // (SIDE * SIDE), (me // SIDE) % SIDE, me % SIDE
    color = (x + y + z) % 2
    pixels = img.shape[1]
    all_pixels = 2 * pixels
    all_samples = 8 * SIDE * SIDE * SIDE

    def at(xx, yy, zz):
        return (xx % SIDE) * (SIDE * SIDE) + (yy % SIDE) * SIDE + zz % SIDE

    line = {
        "z": [at(x, y, z + k) for k in (1, 2, 3)],
        "y": [at(x, y + k, z) for k in (1, 2, 3)],
        "x": [at(x + k, y, z) for k in (1, 2, 3)],
    }
    near = [
        at(x + 1, y, z), at(x + 3, y, z), at(x, y + 1, z),
        at(x, y + 3, z), at(x, y, z + 1), at(x, y, z + 3),
    ]

    barrier = pltpu.get_barrier_semaphore()
    pl.semaphore_signal(barrier, inc=1, device_id=(me, 1 - t), device_id_type=MESH)
    for axis in ("x", "y", "z"):
        for other in line[axis]:
            pl.semaphore_signal(barrier, inc=1, device_id=(other, t), device_id_type=MESH)

    def slabs(p):
        return 2 * p, 2 * p + 1, 2 - p, 3 - 3 * p

    own = slabs(color)
    height = wv.shape[1]
    step = 512
    chunks = pixels // step

    def load(src, dst, k):
        return pltpu.make_async_copy(src, dst, in_sem.at[k])

    def w_rows(k):
        return pl.ds(pl.multiple_of(own[k] * height, height), height)

    load_pls, load_b = load(pls, pv, 0), load(b_out, bv, 1)
    half = pixels // 2
    load_w0 = [
        load(w_out.at[w_rows(0), pl.ds(k * half, half)], wv.at[0, :, pl.ds(k * half, half)], 2 + k)
        for k in range(2)
    ]
    load_img = load(images, img, 4)
    load_w = [load(w_out.at[w_rows(k), :], wv.at[k], 4 + k) for k in (1, 2, 3)]
    load_in = [load(w_in, wbuf.at[t], 8), load(b_in, bbuf.at[t], 9)]
    load_lat = [load(noise, nz, 10), load(enc_mean, em, 11), load(enc_ls, el, 12)]
    for c in [load_pls, load_w0[0], load_w0[1], load_b, load_img, load_w[0]]:
        c.start()
    for c in load_in + load_lat + load_w[1:]:
        c.start()

    def piece(c):
        return slice(c * step, (c + 1) * step)

    def scale(k, c):
        for q in range(2):
            cols = slice(c * step + q * 256, c * step + (q + 1) * 256)
            ws[k, :, cols] = wv[k, :, cols] * s2v[:, cols].astype(BF16)

    def differences(c):
        for q in range(2):
            cols = slice(c * step + q * 256, c * step + (q + 1) * 256)
            d = img[:, cols].astype(F32) - bv[:, cols]
            e = d * s2v[:, cols]
            hi = e.astype(BF16)
            dv[0:128, cols] = hi
            dv[128:256, cols] = (e - hi.astype(F32)).astype(BF16)
            sq = d * e
            acc_sq[...] += sq[:, 0:128] + sq[:, 128:256]

    def nt(a, b):
        return lax.dot_general(a, b, NT, preferred_element_type=F32)

    def block(body):
        pl.when(t < 2)(body)

    def plus(total, more):
        return more if total is None else total + more

    def two_grams(first, second, beside):
        a = b = None
        for c in range(chunks):
            cols = piece(c)
            a = plus(a, nt(first[0][first[1], :, cols], first[2](cols)))
            b = plus(b, nt(second[0][second[1], :, cols], second[2](cols)))
            beside(c)
        return a, b

    def exchange(q):
        out = []
        for d in range(6):
            lo, n = G_ROWS[d] if q < 5 else C_ROWS[d]
            mine = gbuf.at[color, q, pl.ds(lo, n), :] if q < 5 else cbuf.at[color, pl.ds(lo, n), :]
            out.append(
                pltpu.make_async_remote_copy(
                    src_ref=mine, dst_ref=mine, send_sem=g_send.at[q, d], recv_sem=g_recv.at[q, d],
                    device_id=(near[d], t), device_id_type=MESH,
                )
            )
        return out

    def arrivals(q):
        out = []
        for d in range(6):
            lo, n = G_ROWS[d] if q < 5 else C_ROWS[d]
            c = 1 - color
            ref = gbuf.at[c, q, pl.ds(lo, n), :] if q < 5 else cbuf.at[c, pl.ds(lo, n), :]
            out.append(
                pltpu.make_async_remote_copy(
                    src_ref=ref, dst_ref=ref, send_sem=g_send.at[q, d], recv_sem=g_recv.at[q, d],
                    device_id=(near[d], t), device_id_type=MESH,
                )
            )
        return out

    all_sends = [exchange(q) for q in range(6)]

    def send(q):
        for c in all_sends[q]:
            c.start()

    load_pls.wait()
    s2v[...] = jnp.exp(-2.0 * pv[...])
    total_ls = jnp.sum(pv[...], axis=1, keepdims=True)
    acc_sq[...] = jnp.zeros_like(acc_sq)
    load_w0[0].wait()
    def half_gram(k):
        def body():
            parts = [None, None]
            first, last = k * (chunks // 2), (k + 1) * (chunks // 2)
            scale(0, first)
            scale(0, first + 1)
            for c in range(first, last):
                parts[c % 2] = plus(parts[c % 2], nt(ws[0, :, piece(c)], wv[0, :, piece(c)]))
                if c + 2 < last:
                    scale(0, c + 2)
            both = parts[0] + parts[1]
            if k == 0:
                g_half[...] = both
            else:
                gbuf[color, 0] = (0.5 * (g_half[...] + both)).astype(BF16)

        block(body)

    half_gram(0)
    load_w0[1].wait()
    half_gram(1)
    for c in load_in:
        c.wait()
    pl.semaphore_wait(barrier, 10)

    def pair_copy(ref, k):
        return pltpu.make_async_remote_copy(
            src_ref=ref, dst_ref=ref, send_sem=pair_send.at[k], recv_sem=pair_recv.at[k],
            device_id=(me, 1 - t), device_id_type=MESH,
        )

    weights, biases = pair_copy(wbuf.at[t], 0), pair_copy(bbuf.at[t], 1)
    weights.start()
    biases.start()
    send(0)
    load_b.wait()
    load_img.wait()
    load_w[0].wait()
    def beside_gram(c):
        if c + 1 < chunks:
            scale(1, c + 1)
        differences(c)

    rhs1 = lambda cols: wv[1, :, cols]

    @block
    def _():
        scale(1, 0)
        g1, g2 = two_grams((ws, 0, rhs1), (ws, 1, rhs1), beside_gram)
        gbuf[color, 1] = g1.astype(BF16)
        gbuf[color, 2] = (0.5 * g2).astype(BF16)

    send(1)
    send(2)
    for c in load_lat:
        c.wait()
    rhs_d = lambda cols: dv[:, cols]

    @block
    def _():
        mean_t = em[...].T
        ls_t = el[...].T
        exp_t = jnp.exp(ls_t)
        ls_sum = jnp.sum(ls_t, axis=0, keepdims=True)
        first_row = lax.broadcasted_iota(jnp.int32, (128, 1024), 0) == 0
        lat[128:256, :] = jnp.where(first_row, 1.0, 0.0).astype(BF16)

        def beside_cross(c):
            if c < 8:
                n_t = nz[pl.ds(c, 128, stride=8), :].T
                l_t = mean_t + exp_t * n_t
                lat[0:128, c * 128 : (c + 1) * 128] = l_t.astype(BF16)
                squares = jnp.sum(n_t * n_t - l_t * l_t, axis=0, keepdims=True)
                pp[c : c + 1, :] = 0.5 * squares + ls_sum

        c1, c2 = two_grams((wv, 0, rhs_d), (wv, 1, rhs_d), beside_cross)
        cbuf[color, 0:256, :] = c1[:, 0:128] + c1[:, 128:256]
        cbuf[color, 256:512, :] = c2[:, 0:128] + c2[:, 128:256]

    send(5)
    pair_copy(wbuf.at[1 - t], 0).wait_recv()
    pair_copy(bbuf.at[1 - t], 1).wait_recv()
    load_w[1].wait()
    load_w[2].wait()
    row0 = lax.broadcasted_iota(jnp.int32, (128, 128), 0) == 0

    def beside_last(c):
        if c < 8:
            k, lo = c // 4, (c % 4) * 128
            rows = slice(c * 128, (c + 1) * 128)
            wat[rows, 0:128] = wbuf[k, :, lo : lo + 128].astype(F32).T.astype(BF16)
            bias = jnp.where(row0, bbuf[k, :, lo : lo + 128].astype(F32), 0.0)
            wat[rows, 128:256] = bias.T.astype(BF16)

    rhs2, rhs3 = (lambda cols: wv[2, :, cols]), (lambda cols: wv[3, :, cols])

    @block
    def _():
        g3, g4 = two_grams((ws, 0, rhs2), (ws, 1, rhs3), beside_last)
        gbuf[color, 3] = g3.astype(BF16)
        gbuf[color, 4] = g4.astype(BF16)

    send(3)
    send(4)
    @block
    def _():
        for k in range(4):
            rows = slice(k * 256, (k + 1) * 256)
            pre = jnp.dot(wat[rows, :], lat[...], preferred_element_type=F32)
            hid[k] = jnp.maximum(pre, 0.0).astype(BF16)


    def apply(p, which):
        o1, o2, x1, x2 = slabs(p)
        for n in range(4):
            cols = slice(n * 256, (n + 1) * 256)

            def long():
                y = jnp.dot(gbuf[p, 0], hid[o1, :, cols], preferred_element_type=F32)
                y += jnp.dot(gbuf[p, 1], hid[o2, :, cols], preferred_element_type=F32)
                return y + jnp.dot(gbuf[p, 3], hid[x1, :, cols], preferred_element_type=F32)

            def short():
                y = jnp.dot(gbuf[p, 2], hid[o2, :, cols], preferred_element_type=F32)
                return y + jnp.dot(gbuf[p, 4], hid[x2, :, cols], preferred_element_type=F32)

            if n % 2 == 0:
                y1 = long()
                y2 = short()
            else:
                y2 = short()
                y1 = long()
            for h in range(2):
                s = 2 * n + h
                part = slice(h * 128, (h + 1) * 128)
                lanes = slice(s * 128, (s + 1) * 128)
                total = jnp.sum(
                    (cbuf[p, 0:256, :] - y1[:, part]) * hid[o1, :, lanes].astype(F32)
                    + (cbuf[p, 256:512, :] - y2[:, part]) * hid[o2, :, lanes].astype(F32),
                    axis=0, keepdims=True,
                )
                if which == 0:
                    lsend[s : s + 1, :] = total
                else:
                    lsend[s : s + 1, :] += total

    block(functools.partial(apply, color, 0))
    image_part = -0.5 * jnp.sum(acc_sq[...].T, axis=0, keepdims=True)
    lsend[8:16, :] = jnp.broadcast_to(image_part - total_ls - pixels * HALF_LOG_TAU, (8, 128))
    for q in (0, 1, 2, 5, 3, 4):
        for c in arrivals(q):
            c.wait_recv()
    block(functools.partial(apply, 1 - color, 1))

    share = pltpu.make_async_remote_copy(
        src_ref=lsend, dst_ref=lrecv, send_sem=pair_send.at[2], recv_sem=pair_recv.at[2],
        device_id=(me, 1 - t), device_id_type=MESH,
    )
    share.start()
    share.wait_recv()
    loglik = lsend[...] + lrecv[...]
    image_term = loglik[8:9, :]
    logw = loglik[0:8, :] + pp[...]
    peak = jnp.max(logw, axis=0, keepdims=True)
    sums = jnp.sum(jnp.exp(logw - peak), axis=0, keepdims=True)
    rounds = []
    for r, axis in enumerate(("z", "y", "x")):
        sbuf[r, 0:1, :] = peak
        sbuf[r, 1:2, :] = sums
        copies = [
            pltpu.make_async_remote_copy(
                src_ref=sbuf.at[r], dst_ref=rbuf.at[r, k], send_sem=x_send.at[r, k],
                recv_sem=x_recv.at[r, k], device_id=(line[axis][k], t), device_id_type=MESH,
            )
            for k in range(3)
        ]
        for c in copies:
            c.start()
        for c in copies:
            c.wait_recv()
        rounds += copies
        top = peak
        for k in range(3):
            top = jnp.maximum(top, rbuf[r, k, 0:1, :])
        sums = sums * jnp.exp(peak - top)
        for k in range(3):
            sums += rbuf[r, k, 1:2, :] * jnp.exp(rbuf[r, k, 0:1, :] - top)
        peak = top
    log_sum = jnp.log(sums)
    log_all = math.log(all_samples)
    bound_ref[...] = (image_term + peak + log_sum - log_all) / all_pixels
    lw_ref[...] = logw - peak - log_sum + log_all

    for c in rounds + [share, weights, biases]:
        c.wait_send()
    for q in range(6):
        for c in all_sends[q]:
            c.wait_send()


def on_device(images, enc_mean, enc_logscale, noise, w_in, b_in, w_out, b_out, pixel_logscale):
    image_count, sample_count, latent_dims = noise.shape
    hidden, pixels = w_out.shape
    height = hidden // 4
    noise = noise.reshape(image_count * sample_count, latent_dims)
    half = w_in.shape[1]
    V = pltpu.VMEM
    bound, lw = pl.pallas_call(
        kernel,
        out_shape=(
            jax.ShapeDtypeStruct((1, image_count), F32),
            jax.ShapeDtypeStruct((sample_count, image_count), F32),
        ),
        in_specs=[pl.BlockSpec(memory_space=pl.ANY)] * 9,
        out_specs=[pl.BlockSpec(memory_space=pltpu.VMEM)] * 2,
        scratch_shapes=[
            V((4, height, pixels), BF16), V((2, height, pixels), BF16), V((image_count, pixels), BF16),
            V((2 * image_count, pixels), BF16), V((1, pixels), F32), V((1, pixels), F32),
            V(noise.shape, F32), V((image_count, latent_dims), F32), V((image_count, latent_dims), F32),
            V((2, latent_dims, half), BF16), V((2, 1, half), BF16), V((hidden, 256), BF16),
            V((256, image_count * sample_count), BF16), V((4, height, image_count * sample_count), BF16),
            V((2, 5, height, height), BF16), V((2, 2 * height, image_count), F32),
            V((height, height), F32), V((1, pixels), F32), V((image_count, 128), F32), V((sample_count, image_count), F32),
            V((16, image_count), F32), V((16, image_count), F32),
            V((3, 8, image_count), F32), V((3, 3, 8, image_count), F32),
            pltpu.SemaphoreType.DMA((13,)), pltpu.SemaphoreType.DMA((6, 6)), pltpu.SemaphoreType.DMA((6, 6)),
            pltpu.SemaphoreType.DMA((3,)), pltpu.SemaphoreType.DMA((3,)),
            pltpu.SemaphoreType.DMA((3, 3)), pltpu.SemaphoreType.DMA((3, 3)),
        ],
        compiler_params=pltpu.CompilerParams(
            collective_id=0, has_side_effects=True, vmem_limit_bytes=60 * 1024 * 1024
        ),
    )(images, enc_mean, enc_logscale, noise, w_in, b_in, w_out, b_out, pixel_logscale)
    return bound.reshape(image_count), lw.T


def solution(mesh):
    pixel_split = P(None, "tp")
    in_specs = (
        pixel_split, P(), P(), P(None, "samp", None),
        pixel_split, pixel_split, pixel_split, pixel_split, pixel_split,
    )
    out_specs = (P(), P(None, "samp"))
    return jax.shard_map(
        on_device, mesh=mesh, in_specs=in_specs, out_specs=out_specs, check_vma=False
    )
```

```python
import functools
import math

import jax
import jax.numpy as jnp
from jax import lax
from jax.experimental import pallas as pl
from jax.experimental.pallas import tpu as pltpu
from jax.sharding import PartitionSpec as P

HALF_LOG_TAU = 0.9189385332046727
MESH = pl.DeviceIdType.MESH
F32 = jnp.float32
BF16 = jnp.bfloat16
NT = (((1,), (1,)), ((), ()))
G_ROWS = ((0, 48), (48, 48), (96, 48), (144, 48), (192, 32), (224, 32))
C_ROWS = ((0, 48), (48, 48), (96, 40), (136, 40), (176, 40), (216, 40))
SIDE = 4
FINAL = pltpu.VMEM


def kernel(
    images, enc_mean, enc_ls, noise, w_in, b_in, w_out, b_out, pls,
    out_ref,
    wv, ws, img, dv, bv, pv, nz, em, el, wbuf, bbuf, wat, lat, hid, gbuf, cbuf,
    g_half, s2v, acc_sq, pp, lsend, lrecv, sbuf, rbuf,
    in_sem, g_send, g_recv, pair_send, pair_recv, x_send, x_recv,
    plane_sem, cube_sem,
):
    me = lax.axis_index("samp")
    t = lax.axis_index("tp")
    x, y, z = me // (SIDE * SIDE), (me // SIDE) % SIDE, me % SIDE
    color = (x + y + z) % 2
    pixels = img.shape[1]
    all_pixels = 2 * pixels
    all_samples = 8 * SIDE * SIDE * SIDE

    def at(xx, yy, zz):
        return (xx % SIDE) * (SIDE * SIDE) + (yy % SIDE) * SIDE + zz % SIDE

    line = {
        "z": [at(x, y, z + k) for k in (1, 2, 3)],
        "y": [at(x, y + k, z) for k in (1, 2, 3)],
        "x": [at(x + k, y, z) for k in (1, 2, 3)],
    }
    near = [
        at(x + 1, y, z), at(x + 3, y, z), at(x, y + 1, z),
        at(x, y + 3, z), at(x, y, z + 1), at(x, y, z + 3),
    ]

    far = [lax.rem(x + k, SIDE) * (SIDE * SIDE) for k in range(SIDE)]
    mid = [lax.rem(y + k, SIDE) * SIDE for k in range(SIDE)]
    low = [lax.rem(z + k, SIDE) for k in range(SIDE)]
    offsets = [(a, b, c) for a in range(SIDE) for b in range(SIDE) for c in range(SIDE)][1:]
    offsets.sort(key=lambda o: -sum(min(k, SIDE - k) for k in o))

    barrier = pltpu.get_barrier_semaphore()
    pl.semaphore_signal(barrier, inc=1, device_id=(me, 1 - t), device_id_type=MESH)
    for axis in ("x", "y", "z"):
        for other in line[axis]:
            pl.semaphore_signal(barrier, inc=1, device_id=(other, t), device_id_type=MESH)

    def slabs(p):
        return 2 * p, 2 * p + 1, 2 - p, 3 - 3 * p

    own = slabs(color)
    height = wv.shape[1]
    step = 512
    chunks = pixels // step

    def load(src, dst, k):
        return pltpu.make_async_copy(src, dst, in_sem.at[k])

    def w_rows(k):
        return pl.ds(pl.multiple_of(own[k] * height, height), height)

    load_pls, load_b = load(pls, pv, 0), load(b_out, bv, 1)
    half = pixels // 2
    load_w0 = [
        load(w_out.at[w_rows(0), pl.ds(k * half, half)], wv.at[0, :, pl.ds(k * half, half)], 2 + k)
        for k in range(2)
    ]
    load_img = load(images, img, 4)
    load_w = [load(w_out.at[w_rows(k), :], wv.at[k], 4 + k) for k in (1, 2, 3)]
    load_in = [load(w_in, wbuf.at[t], 8), load(b_in, bbuf.at[t], 9)]
    load_lat = [load(noise, nz, 10), load(enc_mean, em, 11), load(enc_ls, el, 12)]
    for c in [load_pls, load_w0[0], load_w0[1], load_w[0], load_w[1], load_w[2], load_b, load_img]:
        c.start()
    for c in load_in + load_lat:
        c.start()

    def piece(c):
        return slice(c * step, (c + 1) * step)

    def scale(k, c):
        for q in range(2):
            cols = slice(c * step + q * 256, c * step + (q + 1) * 256)
            ws[k, :, cols] = wv[k, :, cols] * s2v[:, cols].astype(BF16)

    def differences(c):
        for q in range(2):
            cols = slice(c * step + q * 256, c * step + (q + 1) * 256)
            d = img[:, cols].astype(F32) - bv[:, cols]
            e = d * s2v[:, cols]
            hi = e.astype(BF16)
            dv[0:128, cols] = hi
            dv[128:256, cols] = (e - hi.astype(F32)).astype(BF16)
            sq = d * e
            acc_sq[...] += sq[:, 0:128] + sq[:, 128:256]

    def nt(a, b):
        return lax.dot_general(a, b, NT, preferred_element_type=F32)

    def block(body):
        pl.when(t < 2)(body)

    def plus(total, more):
        return more if total is None else total + more

    def two_grams(first, second, beside):
        a = b = None
        for c in range(chunks):
            cols = piece(c)
            a = plus(a, nt(first[0][first[1], :, cols], first[2](cols)))
            b = plus(b, nt(second[0][second[1], :, cols], second[2](cols)))
            beside(c)
        return a, b

    def part(c, q, lo, n):
        if q < 5:
            return gbuf.at[c, q, pl.ds(lo, n), :]
        return cbuf.at[c, pl.ds((q - 5) * height + lo, n), :]

    def exchange(q):
        out = []
        for d in range(6):
            lo, n = G_ROWS[d] if q < 5 else C_ROWS[d]
            mine = part(color, q, lo, n)
            out.append(
                pltpu.make_async_remote_copy(
                    src_ref=mine, dst_ref=mine, send_sem=g_send.at[q, d], recv_sem=g_recv.at[q, d],
                    device_id=(near[d], t), device_id_type=MESH,
                )
            )
        return out

    def arrivals(q):
        out = []
        for d in range(6):
            lo, n = G_ROWS[d] if q < 5 else C_ROWS[d]
            ref = part(1 - color, q, lo, n)
            out.append(
                pltpu.make_async_remote_copy(
                    src_ref=ref, dst_ref=ref, send_sem=g_send.at[q, d], recv_sem=g_recv.at[q, d],
                    device_id=(near[d], t), device_id_type=MESH,
                )
            )
        return out

    all_sends = [exchange(q) for q in range(7)]

    def send(q):
        for c in all_sends[q]:
            c.start()

    load_pls.wait()
    s2v[...] = jnp.exp(-2.0 * pv[...])
    total_ls = jnp.sum(pv[...], axis=1, keepdims=True)
    acc_sq[...] = jnp.zeros_like(acc_sq)
    load_w0[0].wait()
    def half_gram(k):
        def body():
            parts = [None, None]
            first, last = k * (chunks // 2), (k + 1) * (chunks // 2)
            scale(0, first)
            scale(0, first + 1)
            for c in range(first, last):
                parts[c % 2] = plus(parts[c % 2], nt(ws[0, :, piece(c)], wv[0, :, piece(c)]))
                if c + 2 < last:
                    scale(0, c + 2)
            both = parts[0] + parts[1]
            if k == 0:
                g_half[...] = both
            else:
                gbuf[color, 0] = (0.5 * (g_half[...] + both)).astype(BF16)

        block(body)

    half_gram(0)
    load_w0[1].wait()
    half_gram(1)
    load_w[0].wait()
    def beside_gram(c):
        if c + 1 < chunks:
            scale(1, c + 1)

    rhs1 = lambda cols: wv[1, :, cols]

    @block
    def _():
        scale(1, 0)
        g1, g2 = two_grams((ws, 0, rhs1), (ws, 1, rhs1), beside_gram)
        gbuf[color, 1] = g1.astype(BF16)
        gbuf[color, 2] = (0.5 * g2).astype(BF16)

    for c in load_in:
        c.wait()
    pl.semaphore_wait(barrier, 10)

    def pair_copy(ref, k):
        return pltpu.make_async_remote_copy(
            src_ref=ref, dst_ref=ref, send_sem=pair_send.at[k], recv_sem=pair_recv.at[k],
            device_id=(me, 1 - t), device_id_type=MESH,
        )

    weights, biases = pair_copy(wbuf.at[t], 0), pair_copy(bbuf.at[t], 1)
    weights.start()
    biases.start()
    for other in line["y"]:
        pl.semaphore_signal(plane_sem, inc=1, device_id=(other, t), device_id_type=MESH)
    send(0)
    send(1)
    send(2)
    load_w[1].wait()
    load_w[2].wait()
    load_b.wait()
    load_img.wait()
    rhs2, rhs3 = (lambda cols: wv[2, :, cols]), (lambda cols: wv[3, :, cols])

    @block
    def _():
        g3, g4 = two_grams((ws, 0, rhs2), (ws, 1, rhs3), differences)
        gbuf[color, 3] = g3.astype(BF16)
        gbuf[color, 4] = g4.astype(BF16)

    send(3)
    send(4)
    pl.semaphore_wait(plane_sem, 3)
    for other in line["z"]:
        pl.semaphore_signal(cube_sem, inc=1, device_id=(other, t), device_id_type=MESH)
    for c in load_lat:
        c.wait()

    def cross(k, beside):
        @block
        def _():
            aside = beside()
            parts = [None, None]
            for c in range(chunks):
                cols = piece(c)
                parts[c % 2] = plus(parts[c % 2], nt(wv[k, :, cols], dv[:, cols]))
                aside(c)
            both = parts[0] + parts[1]
            cbuf[color, k * 256 : (k + 1) * 256, :] = both[:, 0:128] + both[:, 128:256]

        send(5 + k)

    def latents():
        mean_t = em[...].T
        ls_t = el[...].T
        exp_t = jnp.exp(ls_t)
        ls_sum = jnp.sum(ls_t, axis=0, keepdims=True)
        first_row = lax.broadcasted_iota(jnp.int32, (128, 1024), 0) == 0
        lat[128:256, :] = jnp.where(first_row, 1.0, 0.0).astype(BF16)

        def aside(c):
            if c < 8:
                n_t = nz[pl.ds(c, 128, stride=8), :].T
                l_t = mean_t + exp_t * n_t
                lat[0:128, c * 128 : (c + 1) * 128] = l_t.astype(BF16)
                squares = jnp.sum(n_t * n_t - l_t * l_t, axis=0, keepdims=True)
                pp[c : c + 1, :] = 0.5 * squares + ls_sum

        return aside

    def projections():
        row0 = lax.broadcasted_iota(jnp.int32, (128, 128), 0) == 0

        def aside(c):
            if c < 8:
                k, lo = c // 4, (c % 4) * 128
                rows = slice(c * 128, (c + 1) * 128)
                wat[rows, 0:128] = wbuf[k, :, lo : lo + 128].astype(F32).T.astype(BF16)
                bias = jnp.where(row0, bbuf[k, :, lo : lo + 128].astype(F32), 0.0)
                wat[rows, 128:256] = bias.T.astype(BF16)

        return aside

    cross(0, latents)
    pair_copy(wbuf.at[1 - t], 0).wait_recv()
    pair_copy(bbuf.at[1 - t], 1).wait_recv()
    cross(1, projections)
    @block
    def _():
        for k in range(4):
            rows = slice(k * 256, (k + 1) * 256)
            pre = jnp.dot(wat[rows, :], lat[...], preferred_element_type=F32)
            hid[k] = jnp.maximum(pre, 0.0).astype(BF16)


    def apply(p, which):
        o1, o2, x1, x2 = slabs(p)
        for n in range(4):
            cols = slice(n * 256, (n + 1) * 256)

            def long():
                y = jnp.dot(gbuf[p, 0], hid[o1, :, cols], preferred_element_type=F32)
                y += jnp.dot(gbuf[p, 1], hid[o2, :, cols], preferred_element_type=F32)
                return y + jnp.dot(gbuf[p, 3], hid[x1, :, cols], preferred_element_type=F32)

            def short():
                y = jnp.dot(gbuf[p, 2], hid[o2, :, cols], preferred_element_type=F32)
                return y + jnp.dot(gbuf[p, 4], hid[x2, :, cols], preferred_element_type=F32)

            if n % 2 == 0:
                y1 = long()
                y2 = short()
            else:
                y2 = short()
                y1 = long()
            for h in range(2):
                s = 2 * n + h
                part = slice(h * 128, (h + 1) * 128)
                lanes = slice(s * 128, (s + 1) * 128)
                total = jnp.sum(
                    (cbuf[p, 0:256, :] - y1[:, part]) * hid[o1, :, lanes].astype(F32)
                    + (cbuf[p, 256:512, :] - y2[:, part]) * hid[o2, :, lanes].astype(F32),
                    axis=0, keepdims=True,
                )
                if which == 0:
                    lsend[s : s + 1, :] = total
                else:
                    lsend[s : s + 1, :] += total

    block(functools.partial(apply, color, 0))
    image_part = -0.5 * jnp.sum(acc_sq[...].T, axis=0, keepdims=True)
    lsend[8:16, :] = jnp.broadcast_to(image_part - total_ls - pixels * HALF_LOG_TAU, (8, 128))
    for q in range(7):
        for c in arrivals(q):
            c.wait_recv()
    block(functools.partial(apply, 1 - color, 1))

    share = pltpu.make_async_remote_copy(
        src_ref=lsend, dst_ref=lrecv, send_sem=pair_send.at[2], recv_sem=pair_recv.at[2],
        device_id=(me, 1 - t), device_id_type=MESH,
    )
    share.start()
    pl.semaphore_wait(cube_sem, 3)
    share.wait_recv()
    loglik = lsend[...] + lrecv[...]
    image_term = loglik[8:9, :]
    logw = loglik[0:8, :] + pp[...]
    peak = jnp.max(logw, axis=0, keepdims=True)
    sums = jnp.sum(jnp.exp(logw - peak), axis=0, keepdims=True)
    sbuf[0:1, :] = peak
    sbuf[1:2, :] = sums
    for k, (a, b, c) in enumerate(offsets):
        pltpu.make_async_remote_copy(
            src_ref=sbuf, dst_ref=rbuf.at[me], send_sem=x_send, recv_sem=x_recv,
            device_id=(far[a] + mid[b] + low[c], t), device_id_type=MESH,
        ).start()
    rbuf[me] = sbuf[...]
    others = rbuf.at[pl.ds(0, len(offsets))]
    pltpu.make_async_copy(others, others, x_recv).wait()
    top = peak
    for k in range(len(offsets) + 1):
        top = jnp.maximum(top, rbuf[k, 0:1, :])
    sums = jnp.zeros_like(peak)
    for k in range(len(offsets) + 1):
        sums += rbuf[k, 1:2, :] * jnp.exp(rbuf[k, 0:1, :] - top)
    log_sum = jnp.log(sums)
    log_all = math.log(all_samples)
    out_ref[0:8, :] = logw - top - log_sum + log_all
    out_ref[8:16, :] = jnp.broadcast_to((image_term + top + log_sum - log_all) / all_pixels, (8, 128))

    pltpu.make_async_copy(others, others, x_send).wait()
    for c in [share, weights, biases]:
        c.wait_send()
    for q in range(7):
        for c in all_sends[q]:
            c.wait_send()


def finish(out_ref, bound_ref, lw_ref):
    bound_ref[...] = out_ref[8:9, :]
    lw_ref[...] = out_ref[0:8, :]


def on_device(images, enc_mean, enc_logscale, noise, w_in, b_in, w_out, b_out, pixel_logscale):
    image_count, sample_count, latent_dims = noise.shape
    hidden, pixels = w_out.shape
    height = hidden // 4
    noise = noise.reshape(image_count * sample_count, latent_dims)
    half = w_in.shape[1]
    V = pltpu.VMEM
    outputs = pl.pallas_call(
        kernel,
        out_shape=FINAL((16, image_count), F32),
        in_specs=[pl.BlockSpec(memory_space=pl.ANY)] * 9,
        out_specs=pl.BlockSpec(memory_space=pltpu.VMEM),
        scratch_shapes=[
            V((4, height, pixels), BF16), V((2, height, pixels), BF16), V((image_count, pixels), BF16),
            V((2 * image_count, pixels), BF16), V((1, pixels), F32), V((1, pixels), F32),
            V(noise.shape, F32), V((image_count, latent_dims), F32), V((image_count, latent_dims), F32),
            V((2, latent_dims, half), BF16), V((2, 1, half), BF16), V((hidden, 256), BF16),
            V((256, image_count * sample_count), BF16), V((4, height, image_count * sample_count), BF16),
            V((2, 5, height, height), BF16), V((2, 2 * height, image_count), F32),
            V((height, height), F32), V((1, pixels), F32), V((image_count, 128), F32), V((sample_count, image_count), F32),
            V((16, image_count), F32), V((16, image_count), F32),
            V((2, image_count), F32), V((64, 2, image_count), F32),
            pltpu.SemaphoreType.DMA((13,)), pltpu.SemaphoreType.DMA((7, 6)), pltpu.SemaphoreType.DMA((7, 6)),
            pltpu.SemaphoreType.DMA((3,)), pltpu.SemaphoreType.DMA((3,)),
            pltpu.SemaphoreType.DMA, pltpu.SemaphoreType.DMA,
            pltpu.SemaphoreType.REGULAR, pltpu.SemaphoreType.REGULAR,
        ],
        compiler_params=pltpu.CompilerParams(
            collective_id=0, has_side_effects=True, vmem_limit_bytes=60 * 1024 * 1024
        ),
    )(images, enc_mean, enc_logscale, noise, w_in, b_in, w_out, b_out, pixel_logscale)
    bound, lw = pl.pallas_call(
        finish,
        out_shape=(
            jax.ShapeDtypeStruct((1, image_count), F32),
            jax.ShapeDtypeStruct((sample_count, image_count), F32),
        ),
        in_specs=[pl.BlockSpec(memory_space=pltpu.VMEM)],
        out_specs=[pl.BlockSpec(memory_space=pltpu.VMEM)] * 2,
    )(pltpu.with_memory_space_constraint(outputs, pltpu.VMEM))
    return bound.reshape(image_count), lw.T


def solution(mesh):
    pixel_split = P(None, "tp")
    in_specs = (
        pixel_split, P(), P(), P(None, "samp", None),
        pixel_split, pixel_split, pixel_split, pixel_split, pixel_split,
    )
    out_specs = (P(), P(None, "samp"))
    return jax.shard_map(
        on_device, mesh=mesh, in_specs=in_specs, out_specs=out_specs, check_vma=False
    )
```

```python
import functools
import math

import jax
import jax.numpy as jnp
from jax import lax
from jax.experimental import pallas as pl
from jax.experimental.pallas import tpu as pltpu
from jax.sharding import PartitionSpec as P

HALF_LOG_TAU = 0.9189385332046727
MESH = pl.DeviceIdType.MESH
F32 = jnp.float32
BF16 = jnp.bfloat16
NT = (((1,), (1,)), ((), ()))
SIDE = 4
FINAL = pltpu.VMEM


def kernel(
    images, enc_mean, enc_ls, noise, w_in, b_in, w_out, b_out, pls,
    out_ref,
    wv, ws, img, dv, bv, pv, nz, em, el, wbuf, bbuf, wat, lat, hid, gbuf, cbuf, lbuf,
    g_half, s2v, acc_sq, pp, lsend, lrecv, sbuf, rbuf,
    in_sem, g_send, g_recv, pair_send, pair_recv, x_send, x_recv,
    plane_sem, cube_sem,
):
    me = lax.axis_index("samp")
    t = lax.axis_index("tp")
    x, y, z = me // (SIDE * SIDE), (me // SIDE) % SIDE, me % SIDE
    color = (x + 2 * y + z) % SIDE
    pixels = img.shape[1]
    all_pixels = 2 * pixels
    all_samples = 8 * SIDE * SIDE * SIDE

    def at(xx, yy, zz):
        return (xx % SIDE) * (SIDE * SIDE) + (yy % SIDE) * SIDE + zz % SIDE

    line = {
        "z": [at(x, y, z + k) for k in (1, 2, 3)],
        "y": [at(x, y + k, z) for k in (1, 2, 3)],
        "x": [at(x + k, y, z) for k in (1, 2, 3)],
    }
    near = [
        at(x + 1, y, z), at(x + 3, y, z), at(x, y + 1, z),
        at(x, y + 3, z), at(x, y, z + 1), at(x, y, z + 3),
    ]

    far = [lax.rem(x + k, SIDE) * (SIDE * SIDE) for k in range(SIDE)]
    mid = [lax.rem(y + k, SIDE) * SIDE for k in range(SIDE)]
    low = [lax.rem(z + k, SIDE) for k in range(SIDE)]
    offsets = [(a, b, c) for a in range(SIDE) for b in range(SIDE) for c in range(SIDE)][1:]
    offsets.sort(key=lambda o: -sum(min(k, SIDE - k) for k in o))

    barrier = pltpu.get_barrier_semaphore()
    pl.semaphore_signal(barrier, inc=1, device_id=(me, 1 - t), device_id_type=MESH)
    for axis in ("x", "y", "z"):
        for other in line[axis]:
            pl.semaphore_signal(barrier, inc=1, device_id=(other, t), device_id_type=MESH)

    own = [lax.rem(color + k, SIDE) for k in range(SIDE)]
    height = wv.shape[1]
    step = 512
    chunks = pixels // step

    def load(src, dst, k):
        return pltpu.make_async_copy(src, dst, in_sem.at[k])

    def w_rows(k):
        return pl.ds(pl.multiple_of(own[k] * height, height), height)

    load_pls, load_b = load(pls, pv, 0), load(b_out, bv, 1)
    half = pixels // 2
    load_w0 = [
        load(w_out.at[w_rows(0), pl.ds(k * half, half)], wv.at[0, :, pl.ds(k * half, half)], 2 + k)
        for k in range(2)
    ]
    load_img = load(images, img, 4)
    load_w = [load(w_out.at[w_rows(k), :], wv.at[k], 4 + k) for k in (1, 2, 3)]
    load_in = [load(w_in, wbuf.at[t], 8), load(b_in, bbuf.at[t], 9)]
    load_lat = [load(noise, nz, 10), load(enc_mean, em, 11), load(enc_ls, el, 12)]
    for c in [load_pls] + load_w0 + load_in + [load_b, load_img] + load_lat + load_w:
        c.start()

    def piece(c):
        return slice(c * step, (c + 1) * step)

    def scale(k, c):
        for q in range(2):
            cols = slice(c * step + q * 256, c * step + (q + 1) * 256)
            ws[k, :, cols] = wv[k, :, cols] * s2v[:, cols].astype(BF16)

    def differences(c):
        for q in range(2):
            cols = slice(c * step + q * 256, c * step + (q + 1) * 256)
            d = img[:, cols].astype(F32) - bv[:, cols]
            e = d * s2v[:, cols]
            hi = e.astype(BF16)
            dv[0:128, cols] = hi
            dv[128:256, cols] = (e - hi.astype(F32)).astype(BF16)
            sq = d * e
            acc_sq[...] += sq[:, 0:128] + sq[:, 128:256]

    def nt(a, b):
        return lax.dot_general(a, b, NT, preferred_element_type=F32)

    def block(body):
        pl.when(t < 2)(body)

    def plus(total, more):
        return more if total is None else total + more

    halves = (0, 0, 0, 1, 1, 1)
    senders = [own[k] for k in (3, 1, 2, 2, 3, 1)]

    def part(c, q, d):
        rows = pl.ds(halves[d] * (height // 2), height // 2)
        return gbuf.at[c, q, rows, :] if q < 2 else cbuf.at[c, rows, :]

    def to_near(ref, q, d):
        return pltpu.make_async_remote_copy(
            src_ref=ref, dst_ref=ref, send_sem=g_send.at[q, d], recv_sem=g_recv.at[q, d],
            device_id=(near[d], t), device_id_type=MESH,
        )

    all_sends = [[to_near(part(color, q, d), q, d) for d in range(6)] for q in range(3)]

    def send(q):
        for c in all_sends[q]:
            c.start()

    def receive(q):
        for d in range(6):
            to_near(part(senders[d], q, d), q, d).wait_recv()

    load_pls.wait()
    s2v[...] = jnp.exp(-2.0 * pv[...])
    total_ls = jnp.sum(pv[...], axis=1, keepdims=True)
    acc_sq[...] = jnp.zeros_like(acc_sq)
    load_w0[0].wait()
    def half_gram(k):
        def body():
            parts = [None, None]
            first, last = k * (chunks // 2), (k + 1) * (chunks // 2)
            scale(0, first)
            scale(0, first + 1)
            for c in range(first, last):
                parts[c % 2] = plus(parts[c % 2], nt(ws[0, :, piece(c)], wv[0, :, piece(c)]))
                if c + 2 < last:
                    scale(0, c + 2)
            both = parts[0] + parts[1]
            if k == 0:
                g_half[...] = both
            else:
                gbuf[color, 0] = (0.5 * (g_half[...] + both)).astype(BF16)

        block(body)

    half_gram(0)
    load_w0[1].wait()
    half_gram(1)
    for c in load_in:
        c.wait()
    pl.semaphore_wait(barrier, 10)

    def pair_copy(ref, k):
        return pltpu.make_async_remote_copy(
            src_ref=ref, dst_ref=ref, send_sem=pair_send.at[k], recv_sem=pair_recv.at[k],
            device_id=(me, 1 - t), device_id_type=MESH,
        )

    weights, biases = pair_copy(wbuf.at[t], 0), pair_copy(bbuf.at[t], 1)
    weights.start()
    biases.start()
    send(0)
    for other in line["y"]:
        pl.semaphore_signal(plane_sem, inc=1, device_id=(other, t), device_id_type=MESH)
    load_b.wait()
    load_img.wait()

    @block
    def _():
        parts = [None, None]
        differences(0)
        differences(1)
        for c in range(chunks):
            cols = piece(c)
            parts[c % 2] = plus(parts[c % 2], nt(wv[0, :, cols], dv[:, cols]))
            if c + 2 < chunks:
                differences(c + 2)
        both = parts[0] + parts[1]
        cbuf[color] = both[:, 0:128] + both[:, 128:256]

    send(2)
    for c in load_lat:
        c.wait()
    load_w[0].wait()

    @block
    def _():
        mean_t = em[...].T
        ls_t = el[...].T
        exp_t = jnp.exp(ls_t)
        ls_sum = jnp.sum(ls_t, axis=0, keepdims=True)
        first_row = lax.broadcasted_iota(jnp.int32, (128, 1024), 0) == 0
        lat[128:256, :] = jnp.where(first_row, 1.0, 0.0).astype(BF16)
        parts = [None, None]
        for c in range(chunks):
            cols = piece(c)
            parts[c % 2] = plus(parts[c % 2], nt(ws[0, :, cols], wv[1, :, cols]))
            if c < 8:
                n_t = nz[pl.ds(c, 128, stride=8), :].T
                l_t = mean_t + exp_t * n_t
                lat[0:128, c * 128 : (c + 1) * 128] = l_t.astype(BF16)
                squares = jnp.sum(n_t * n_t - l_t * l_t, axis=0, keepdims=True)
                pp[c : c + 1, :] = 0.5 * squares + ls_sum
        gbuf[color, 1] = (parts[0] + parts[1]).astype(BF16)

    send(1)
    pl.semaphore_wait(plane_sem, 3)
    for other in line["z"]:
        pl.semaphore_signal(cube_sem, inc=1, device_id=(other, t), device_id_type=MESH)
    pair_copy(wbuf.at[1 - t], 0).wait_recv()
    pair_copy(bbuf.at[1 - t], 1).wait_recv()
    load_w[1].wait()
    load_w[2].wait()

    @block
    def _():
        row0 = lax.broadcasted_iota(jnp.int32, (128, 128), 0) == 0
        l0 = l1 = None
        scale(1, 0)
        for c in range(chunks):
            cols = piece(c)
            l0 = plus(l0, nt(ws[0, :, cols], wv[2, :, cols]))
            l1 = plus(l1, nt(ws[1, :, cols], wv[3, :, cols]))
            if c + 1 < chunks:
                scale(1, c + 1)
            if c < 8:
                k, lo = c // 4, (c % 4) * 128
                rows = slice(c * 128, (c + 1) * 128)
                wat[rows, 0:128] = wbuf[k, :, lo : lo + 128].astype(F32).T.astype(BF16)
                bias = jnp.where(row0, bbuf[k, :, lo : lo + 128].astype(F32), 0.0)
                wat[rows, 128:256] = bias.T.astype(BF16)
        lbuf[0] = l0.astype(BF16)
        lbuf[1] = l1.astype(BF16)

    @block
    def _():
        for k in range(4):
            rows = slice(k * 256, (k + 1) * 256)
            pre = jnp.dot(wat[rows, :], lat[...], preferred_element_type=F32)
            hid[k] = jnp.maximum(pre, 0.0).astype(BF16)


    def against(ref, k, cols):
        return jnp.dot(ref, hid[own[k], :, cols], preferred_element_type=F32)

    def weigh(y, k, cols):
        h = hid[own[k], :, cols].astype(F32)
        c = cbuf[own[k]]
        return jnp.sum((jnp.concatenate([c, c], axis=1) - y) * h, axis=0, keepdims=True)

    def rows_of(total, n, first):
        for h in range(2):
            s = 2 * n + h
            lanes = total[:, h * 128 : (h + 1) * 128]
            if first:
                lsend[s : s + 1, :] = lanes
            else:
                lsend[s : s + 1, :] += lanes

    @block
    def _():
        for n in range(4):
            cols = slice(n * 256, (n + 1) * 256)

            def two(first, k, second, j):
                return against(first, k, cols) + against(second, j, cols)

            y = two(gbuf[color, 0], 0, gbuf[color, 1], 1)
            w = against(lbuf[0], 2, cols)
            v = against(lbuf[1], 3, cols)
            far_part = jnp.sum(v * hid[own[1], :, cols].astype(F32), axis=0, keepdims=True)
            rows_of(weigh(y + w, 0, cols) - far_part, n, True)

    image_part = -0.5 * jnp.sum(acc_sq[...].T, axis=0, keepdims=True)
    lsend[8:16, :] = jnp.broadcast_to(image_part - total_ls - pixels * HALF_LOG_TAU, (8, 128))
    for q in (0, 2, 1):
        receive(q)

    @block
    def _():
        for n in range(4):
            cols = slice(n * 256, (n + 1) * 256)
            total = None
            for k in (1, 2, 3):
                c = own[k]
                y = against(gbuf[c, 0], k, cols) + against(gbuf[c, 1], (k + 1) % 4, cols)
                total = plus(total, weigh(y, k, cols))
            rows_of(total, n, False)

    share = pltpu.make_async_remote_copy(
        src_ref=lsend, dst_ref=lrecv, send_sem=pair_send.at[2], recv_sem=pair_recv.at[2],
        device_id=(me, 1 - t), device_id_type=MESH,
    )
    share.start()
    pl.semaphore_wait(cube_sem, 3)
    share.wait_recv()
    loglik = lsend[...] + lrecv[...]
    image_term = loglik[8:9, :]
    logw = loglik[0:8, :] + pp[...]
    peak = jnp.max(logw, axis=0, keepdims=True)
    sums = jnp.sum(jnp.exp(logw - peak), axis=0, keepdims=True)
    sbuf[0:1, :] = peak
    sbuf[1:2, :] = sums
    for k, (a, b, c) in enumerate(offsets):
        pltpu.make_async_remote_copy(
            src_ref=sbuf, dst_ref=rbuf.at[me], send_sem=x_send, recv_sem=x_recv,
            device_id=(far[a] + mid[b] + low[c], t), device_id_type=MESH,
        ).start()
    rbuf[me] = sbuf[...]
    others = rbuf.at[pl.ds(0, len(offsets))]
    pltpu.make_async_copy(others, others, x_recv).wait()
    top = peak
    for k in range(len(offsets) + 1):
        top = jnp.maximum(top, rbuf[k, 0:1, :])
    sums = jnp.zeros_like(peak)
    for k in range(len(offsets) + 1):
        sums += rbuf[k, 1:2, :] * jnp.exp(rbuf[k, 0:1, :] - top)
    log_sum = jnp.log(sums)
    log_all = math.log(all_samples)
    out_ref[0:8, :] = logw - top - log_sum + log_all
    out_ref[8:16, :] = jnp.broadcast_to((image_term + top + log_sum - log_all) / all_pixels, (8, 128))

    pltpu.make_async_copy(others, others, x_send).wait()
    for c in [share, weights, biases]:
        c.wait_send()
    for q in range(3):
        for c in all_sends[q]:
            c.wait_send()


def finish(out_ref, bound_ref, lw_ref):
    bound_ref[...] = out_ref[8:9, :]
    lw_ref[...] = out_ref[0:8, :]


def on_device(images, enc_mean, enc_logscale, noise, w_in, b_in, w_out, b_out, pixel_logscale):
    image_count, sample_count, latent_dims = noise.shape
    hidden, pixels = w_out.shape
    height = hidden // 4
    noise = noise.reshape(image_count * sample_count, latent_dims)
    half = w_in.shape[1]
    V = pltpu.VMEM
    outputs = pl.pallas_call(
        kernel,
        out_shape=FINAL((16, image_count), F32),
        in_specs=[pl.BlockSpec(memory_space=pl.ANY)] * 9,
        out_specs=pl.BlockSpec(memory_space=pltpu.VMEM),
        scratch_shapes=[
            V((4, height, pixels), BF16), V((2, height, pixels), BF16), V((image_count, pixels), BF16),
            V((2 * image_count, pixels), BF16), V((1, pixels), F32), V((1, pixels), F32),
            V(noise.shape, F32), V((image_count, latent_dims), F32), V((image_count, latent_dims), F32),
            V((2, latent_dims, half), BF16), V((2, 1, half), BF16), V((hidden, 256), BF16),
            V((256, image_count * sample_count), BF16), V((4, height, image_count * sample_count), BF16),
            V((4, 2, height, height), BF16), V((4, height, image_count), F32), V((2, height, height), BF16),
            V((height, height), F32), V((1, pixels), F32), V((image_count, 128), F32), V((sample_count, image_count), F32),
            V((16, image_count), F32), V((16, image_count), F32),
            V((2, image_count), F32), V((64, 2, image_count), F32),
            pltpu.SemaphoreType.DMA((13,)), pltpu.SemaphoreType.DMA((3, 6)), pltpu.SemaphoreType.DMA((3, 6)),
            pltpu.SemaphoreType.DMA((3,)), pltpu.SemaphoreType.DMA((3,)),
            pltpu.SemaphoreType.DMA, pltpu.SemaphoreType.DMA,
            pltpu.SemaphoreType.REGULAR, pltpu.SemaphoreType.REGULAR,
        ],
        compiler_params=pltpu.CompilerParams(
            collective_id=0, has_side_effects=True, vmem_limit_bytes=60 * 1024 * 1024
        ),
    )(images, enc_mean, enc_logscale, noise, w_in, b_in, w_out, b_out, pixel_logscale)
    bound, lw = pl.pallas_call(
        finish,
        out_shape=(
            jax.ShapeDtypeStruct((1, image_count), F32),
            jax.ShapeDtypeStruct((sample_count, image_count), F32),
        ),
        in_specs=[pl.BlockSpec(memory_space=pltpu.VMEM)],
        out_specs=[pl.BlockSpec(memory_space=pltpu.VMEM)] * 2,
    )(pltpu.with_memory_space_constraint(outputs, pltpu.VMEM))
    return bound.reshape(image_count), lw.T


def solution(mesh):
    pixel_split = P(None, "tp")
    in_specs = (
        pixel_split, P(), P(), P(None, "samp", None),
        pixel_split, pixel_split, pixel_split, pixel_split, pixel_split,
    )
    out_specs = (P(), P(None, "samp"))
    return jax.shard_map(
        on_device, mesh=mesh, in_specs=in_specs, out_specs=out_specs, check_vma=False
    )
```

```python
import functools
import math

import jax
import jax.numpy as jnp
from jax import lax
from jax.experimental import pallas as pl
from jax.experimental.pallas import tpu as pltpu
from jax.sharding import PartitionSpec as P

HALF_LOG_TAU = 0.9189385332046727
MESH = pl.DeviceIdType.MESH
F32 = jnp.float32
BF16 = jnp.bfloat16
NT = (((1,), (1,)), ((), ()))
SIDE = 4
FINAL = pltpu.VMEM


def kernel(
    images, enc_mean, enc_ls, noise, w_in, b_in, w_out, b_out, pls,
    out_ref,
    wv, ws, img, dv, row, nz, wbuf, bbuf, wat, lat, hid, gbuf, cbuf, lbuf,
    g_part, s2v, acc_sq, pp, lsend, lrecv, sbuf, rbuf,
    in_sem, g_send, g_recv, pair_send, pair_recv, x_send, x_recv,
    plane_sem, cube_sem,
):
    me = lax.axis_index("samp")
    t = lax.axis_index("tp")
    x, y, z = me // (SIDE * SIDE), (me // SIDE) % SIDE, me % SIDE
    color = (x + 2 * y + z) % SIDE
    pixels = img.shape[1]
    all_pixels = 2 * pixels
    all_samples = 8 * SIDE * SIDE * SIDE

    def at(xx, yy, zz):
        return (xx % SIDE) * (SIDE * SIDE) + (yy % SIDE) * SIDE + zz % SIDE

    line = {
        "z": [at(x, y, z + k) for k in (1, 2, 3)],
        "y": [at(x, y + k, z) for k in (1, 2, 3)],
        "x": [at(x + k, y, z) for k in (1, 2, 3)],
    }
    near = [
        at(x + 1, y, z), at(x + 3, y, z), at(x, y + 1, z),
        at(x, y + 3, z), at(x, y, z + 1), at(x, y, z + 3),
    ]

    far = [lax.rem(x + k, SIDE) * (SIDE * SIDE) for k in range(SIDE)]
    mid = [lax.rem(y + k, SIDE) * SIDE for k in range(SIDE)]
    low = [lax.rem(z + k, SIDE) for k in range(SIDE)]
    offsets = [(a, b, c) for a in range(SIDE) for b in range(SIDE) for c in range(SIDE)][1:]
    offsets.sort(key=lambda o: sum((k + 3) % SIDE for k in o))

    own = [lax.rem(color + k, SIDE) for k in range(SIDE)]
    height = wv.shape[1]
    step = 512
    chunks = pixels // step

    def load(src, dst, k):
        return pltpu.make_async_copy(src, dst, in_sem.at[k])

    def w_rows(k):
        return pl.ds(pl.multiple_of(own[k] * height, height), height)

    cuts = (0, 2, 6, chunks)
    load_row = [load(pls, row.at[0], 0), load(b_out, row.at[1], 0)]
    load_first = [
        load(
            w_out.at[w_rows(0), pl.ds(cuts[k] * step, (cuts[k + 1] - cuts[k]) * step)],
            wv.at[0, :, pl.ds(cuts[k] * step, (cuts[k + 1] - cuts[k]) * step)],
            1 + k,
        )
        for k in range(3)
    ]
    load_in = [load(w_in, wbuf.at[t], 4), load(b_in, bbuf.at[t], 5)]
    load_img = load(images, img, 6)
    images_n, samples_n = enc_mean.shape[0], noise.shape[0]
    load_lat = [
        load(noise, nz.at[pl.ds(0, samples_n), :], 7),
        load(enc_mean, nz.at[pl.ds(samples_n, images_n), :], 7),
        load(enc_ls, nz.at[pl.ds(samples_n + images_n, images_n), :], 7),
    ]
    load_w = [load(w_out.at[w_rows(k), :], wv.at[k], (8, 9, 9)[k - 1]) for k in (1, 2, 3)]
    for c in load_row + load_first + load_in + [load_img] + load_lat + load_w:
        c.start()

    barrier = pltpu.get_barrier_semaphore()
    pl.semaphore_signal(barrier, inc=1, device_id=(me, 1 - t), device_id_type=MESH)
    for axis in ("x", "y", "z"):
        for other in line[axis]:
            pl.semaphore_signal(barrier, inc=1, device_id=(other, t), device_id_type=MESH)

    def piece(c):
        return slice(c * step, (c + 1) * step)

    def scale(k, c):
        for q in range(2):
            cols = slice(c * step + q * 256, c * step + (q + 1) * 256)
            ws[k, :, cols] = wv[k, :, cols] * s2v[:, cols].astype(BF16)

    def differences(q):
        cols = slice(q * 256, (q + 1) * 256)
        e = (img[:, cols].astype(F32) - row[1, :, cols]) * s2v[:, cols]
        hi = e.astype(BF16)
        dv[0:128, cols] = hi
        dv[128:256, cols] = (e - hi.astype(F32)).astype(BF16)

    def squares(c):
        for q in range(2):
            cols = slice(c * step + q * 256, c * step + (q + 1) * 256)
            d = img[:, cols].astype(F32) - row[1, :, cols]
            sq = d * d * s2v[:, cols]
            acc_sq[...] += sq[:, 0:128] + sq[:, 128:256]

    def project(k, lo):
        rows = slice(lo, lo + 128)
        row0 = lax.broadcasted_iota(jnp.int32, (128, 128), 0) == 0
        wat[k, rows, 0:128] = wbuf[k, :, rows].astype(F32).T.astype(BF16)
        wat[k, rows, 128:256] = jnp.where(row0, bbuf[k, :, rows].astype(F32), 0.0).T.astype(BF16)

    def nt(a, b):
        return lax.dot_general(a, b, NT, preferred_element_type=F32)

    def block(body):
        pl.when(t < 2)(body)

    def plus(total, more):
        return more if total is None else total + more

    halves = (0, 0, 0, 1, 1, 1)
    senders = [own[k] for k in (3, 1, 2, 2, 3, 1)]

    def part(c, q, d):
        rows = pl.ds(halves[d] * (height // 2), height // 2)
        return gbuf.at[c, q, rows, :] if q < 2 else cbuf.at[c, rows, :]

    def to_near(ref, q, d):
        return pltpu.make_async_remote_copy(
            src_ref=ref, dst_ref=ref, send_sem=g_send, recv_sem=g_recv.at[q],
            device_id=(near[d], t), device_id_type=MESH,
        )

    all_sends = [[to_near(part(color, q, d), q, d) for d in range(6)] for q in range(3)]

    def send(q):
        for c in all_sends[q]:
            c.start()

    def wait_bytes(ref, sem):
        pltpu.make_async_copy(ref, ref, sem).wait()

    def receive(q):
        wait_bytes(gbuf.at[pl.ds(0, 3), q] if q < 2 else cbuf.at[pl.ds(0, 3)], g_recv.at[q])

    wait_bytes(row, in_sem.at[0])
    s2v[...] = jnp.exp(-2.0 * row[0])
    total_ls = jnp.sum(row[0], axis=1, keepdims=True)
    acc_sq[...] = jnp.zeros_like(acc_sq)
    load_first[0].wait()
    def part_gram(k):
        def body():
            parts = [None, None]
            first, last = cuts[k], cuts[k + 1]
            scale(0, first)
            scale(0, first + 1)
            for c in range(first, last):
                parts[c % 2] = plus(parts[c % 2], nt(ws[0, :, piece(c)], wv[0, :, piece(c)]))
                if c + 2 < last:
                    scale(0, c + 2)
            both = parts[0] + parts[1]
            if k == 0:
                g_part[...] = both
            elif k == 1:
                g_part[...] += both
            else:
                gbuf[color, 0] = (0.5 * (g_part[...] + both)).astype(BF16)

        block(body)

    part_gram(0)
    load_first[1].wait()
    part_gram(1)
    load_first[2].wait()
    part_gram(2)
    for c in load_in:
        c.wait()
    pl.semaphore_wait(barrier, 10)

    def pair_copy(ref, k):
        return pltpu.make_async_remote_copy(
            src_ref=ref, dst_ref=ref, send_sem=pair_send.at[k], recv_sem=pair_recv.at[k],
            device_id=(me, 1 - t), device_id_type=MESH,
        )

    weights, biases = pair_copy(wbuf.at[t], 0), pair_copy(bbuf.at[t], 1)
    weights.start()
    biases.start()
    send(0)
    for other in line["y"]:
        pl.semaphore_signal(plane_sem, inc=1, device_id=(other, t), device_id_type=MESH)
    load_img.wait()

    @block
    def _():
        parts = [None, None]
        lead = 2
        for q in range(lead):
            differences(q)
        for q in range(2 * chunks):
            cols = slice(q * 256, (q + 1) * 256)
            parts[q % 2] = plus(parts[q % 2], nt(wv[0, :, cols], dv[:, cols]))
            if q + lead < 2 * chunks:
                differences(q + lead)
            if q % 5 == 2 and q // 5 < 4:
                project(t, (q // 5) * 128)
        both = parts[0] + parts[1]
        cbuf[color] = both[:, 0:128] + both[:, 128:256]

    send(2)
    wait_bytes(nz, in_sem.at[7])
    load_w[0].wait()


    @block
    def _():
        parts = [None, None]
        for c in range(chunks):
            cols = piece(c)
            parts[c % 2] = plus(parts[c % 2], nt(ws[0, :, cols], wv[1, :, cols]))
            if c == 0:
                mean_t = nz[samples_n : samples_n + images_n, :].T
                ls_t = nz[samples_n + images_n :, :].T
                exp_t = jnp.exp(ls_t)
                ls_sum = jnp.sum(ls_t, axis=0, keepdims=True)
                first_row = lax.broadcasted_iota(jnp.int32, (128, 1024), 0) == 0
                lat[128:256, :] = jnp.where(first_row, 1.0, 0.0).astype(BF16)
            elif c < 9:
                i = c - 1
                n_t = nz[pl.ds(i, 128, stride=8), :].T
                l_t = mean_t + exp_t * n_t
                lat[0:128, i * 128 : (i + 1) * 128] = l_t.astype(BF16)
                total = jnp.sum(n_t * n_t - l_t * l_t, axis=0, keepdims=True)
                pp[i : i + 1, :] = 0.5 * total + ls_sum
            else:
                squares(c)
        gbuf[color, 1] = (parts[0] + parts[1]).astype(BF16)

    pl.when(t == 0)(functools.partial(send, 1))
    pl.semaphore_wait(plane_sem, 3)
    for other in line["z"]:
        pl.semaphore_signal(cube_sem, inc=1, device_id=(other, t), device_id_type=MESH)
    def hide(k):
        for j in range(2):
            rows = slice(j * 256, (j + 1) * 256)
            pre = jnp.dot(wat[k, rows, :], lat[...], preferred_element_type=F32)
            hid[2 * k + j] = jnp.maximum(pre, 0.0).astype(BF16)

    block(functools.partial(hide, t))
    pl.when(t == 1)(functools.partial(send, 1))
    wait_bytes(wv.at[pl.ds(2, 2)], in_sem.at[9])
    pair_copy(wbuf.at[1 - t], 0).wait_recv()
    pair_copy(bbuf.at[1 - t], 1).wait_recv()

    @block
    def _():
        l0 = l1 = None
        scale(1, 0)
        for c in range(chunks):
            cols = piece(c)
            l0 = plus(l0, nt(ws[0, :, cols], wv[2, :, cols]))
            l1 = plus(l1, nt(ws[1, :, cols], wv[3, :, cols]))
            if c + 1 < chunks:
                scale(1, c + 1)
            if c < 4:
                project(1 - t, c * 128)
            if c < 9:
                squares(c)
        lbuf[0] = l0.astype(BF16)
        lbuf[1] = l1.astype(BF16)


    block(functools.partial(hide, 1 - t))

    def against(ref, k, cols):
        return jnp.dot(ref, hid[own[k], :, cols], preferred_element_type=F32)

    def weigh(y, k, cols):
        h = hid[own[k], :, cols].astype(F32)
        c = cbuf[own[k]]
        return jnp.sum((jnp.concatenate([c, c], axis=1) - y) * h, axis=0, keepdims=True)

    def rows_of(total, n, first):
        for h in range(2):
            s = 2 * n + h
            lanes = total[:, h * 128 : (h + 1) * 128]
            if first:
                lsend[s : s + 1, :] = lanes
            else:
                lsend[s : s + 1, :] += lanes

    @block
    def _():
        for n in range(4):
            cols = slice(n * 256, (n + 1) * 256)

            def two(first, k, second, j):
                return against(first, k, cols) + against(second, j, cols)

            y = two(gbuf[color, 0], 0, gbuf[color, 1], 1)
            w = against(lbuf[0], 2, cols)
            v = against(lbuf[1], 3, cols)
            far_part = jnp.sum(v * hid[own[1], :, cols].astype(F32), axis=0, keepdims=True)
            rows_of(weigh(y + w, 0, cols) - far_part, n, True)

    image_part = -0.5 * jnp.sum(acc_sq[...].T, axis=0, keepdims=True)
    lsend[8:16, :] = jnp.broadcast_to(image_part - total_ls - pixels * HALF_LOG_TAU, (8, 128))
    receive(0)
    receive(2)

    @block
    def _():
        for n in range(4):
            cols = slice(n * 256, (n + 1) * 256)
            total = None
            for k in (1, 2, 3):
                total = plus(total, weigh(against(gbuf[own[k], 0], k, cols), k, cols))
            rows_of(total, n, False)

    receive(1)

    @block
    def _():
        for n in range(4):
            cols = slice(n * 256, (n + 1) * 256)
            total = None
            for k in (1, 2, 3):
                y = against(gbuf[own[k], 1], (k + 1) % 4, cols) * hid[own[k], :, cols].astype(F32)
                total = plus(total, jnp.sum(y, axis=0, keepdims=True))
            rows_of(-total, n, False)

    share = pltpu.make_async_remote_copy(
        src_ref=lsend, dst_ref=lrecv, send_sem=pair_send.at[2], recv_sem=pair_recv.at[2],
        device_id=(me, 1 - t), device_id_type=MESH,
    )
    share.start()
    pl.semaphore_wait(cube_sem, 3)
    share.wait_recv()
    loglik = lsend[...] + lrecv[...]
    image_term = loglik[8:9, :]
    logw = loglik[0:8, :] + pp[...]
    peak = jnp.max(logw, axis=0, keepdims=True)
    sums = jnp.sum(jnp.exp(logw - peak), axis=0, keepdims=True)
    sbuf[0:1, :] = peak
    sbuf[1:2, :] = sums
    for k, (a, b, c) in enumerate(offsets):
        pltpu.make_async_remote_copy(
            src_ref=sbuf, dst_ref=rbuf.at[me], send_sem=x_send, recv_sem=x_recv,
            device_id=(far[a] + mid[b] + low[c], t), device_id_type=MESH,
        ).start()
    rbuf[me] = sbuf[...]
    others = rbuf.at[pl.ds(0, len(offsets))]
    pltpu.make_async_copy(others, others, x_recv).wait()
    top = peak
    for k in range(len(offsets) + 1):
        top = jnp.maximum(top, rbuf[k, 0:1, :])
    sums = jnp.zeros_like(peak)
    for k in range(len(offsets) + 1):
        sums += rbuf[k, 1:2, :] * jnp.exp(rbuf[k, 0:1, :] - top)
    log_sum = jnp.log(sums)
    log_all = math.log(all_samples)
    out_ref[0:8, :] = logw - top - log_sum + log_all
    out_ref[8:16, :] = jnp.broadcast_to((image_term + top + log_sum - log_all) / all_pixels, (8, 128))

    pltpu.make_async_copy(others, others, x_send).wait()
    for c in [share, weights, biases]:
        c.wait_send()
    wait_bytes(ws.at[0, pl.ds(0, 96), :], g_send)


def finish(out_ref, bound_ref, lw_ref, sems):
    copies = [
        pltpu.make_async_copy(out_ref.at[pl.ds(0, 8), :], lw_ref, sems.at[0]),
        pltpu.make_async_copy(out_ref.at[pl.ds(8, 1), :], bound_ref, sems.at[1]),
    ]
    for c in copies:
        c.start()
    for c in copies:
        c.wait()


def on_device(images, enc_mean, enc_logscale, noise, w_in, b_in, w_out, b_out, pixel_logscale):
    image_count, sample_count, latent_dims = noise.shape
    hidden, pixels = w_out.shape
    height = hidden // 4
    noise = noise.reshape(image_count * sample_count, latent_dims)
    half = w_in.shape[1]
    V = pltpu.VMEM
    outputs = pl.pallas_call(
        kernel,
        out_shape=FINAL((16, image_count), F32),
        in_specs=[pl.BlockSpec(memory_space=pl.ANY)] * 9,
        out_specs=pl.BlockSpec(memory_space=pltpu.VMEM),
        scratch_shapes=[
            V((4, height, pixels), BF16), V((2, height, pixels), BF16), V((image_count, pixels), BF16),
            V((2 * image_count, pixels), BF16), V((2, 1, pixels), F32),
            V((noise.shape[0] + 2 * image_count, latent_dims), F32),
            V((2, latent_dims, half), BF16), V((2, 1, half), BF16), V((2, half, 256), BF16),
            V((256, image_count * sample_count), BF16), V((4, height, image_count * sample_count), BF16),
            V((4, 2, height, height), BF16), V((4, height, image_count), F32), V((2, height, height), BF16),
            V((height, height), F32), V((1, pixels), F32), V((image_count, 128), F32), V((sample_count, image_count), F32),
            V((16, image_count), F32), V((16, image_count), F32),
            V((2, image_count), F32), V((64, 2, image_count), F32),
            pltpu.SemaphoreType.DMA((10,)), pltpu.SemaphoreType.DMA, pltpu.SemaphoreType.DMA((3,)),
            pltpu.SemaphoreType.DMA((3,)), pltpu.SemaphoreType.DMA((3,)),
            pltpu.SemaphoreType.DMA, pltpu.SemaphoreType.DMA,
            pltpu.SemaphoreType.REGULAR, pltpu.SemaphoreType.REGULAR,
        ],
        compiler_params=pltpu.CompilerParams(
            collective_id=0, has_side_effects=True, vmem_limit_bytes=60 * 1024 * 1024
        ),
    )(images, enc_mean, enc_logscale, noise, w_in, b_in, w_out, b_out, pixel_logscale)
    bound, lw = pl.pallas_call(
        finish,
        out_shape=(
            jax.ShapeDtypeStruct((1, image_count), F32),
            jax.ShapeDtypeStruct((sample_count, image_count), F32),
        ),
        in_specs=[pl.BlockSpec(memory_space=pltpu.VMEM)],
        out_specs=[pl.BlockSpec(memory_space=pl.ANY)] * 2,
        scratch_shapes=[pltpu.SemaphoreType.DMA((2,))],
    )(pltpu.with_memory_space_constraint(outputs, pltpu.VMEM))
    return bound.reshape(image_count), lw.T


def solution(mesh):
    pixel_split = P(None, "tp")
    in_specs = (
        pixel_split, P(), P(), P(None, "samp", None),
        pixel_split, pixel_split, pixel_split, pixel_split, pixel_split,
    )
    out_specs = (P(), P(None, "samp"))
    return jax.shard_map(
        on_device, mesh=mesh, in_specs=in_specs, out_specs=out_specs, check_vma=False
    )
```
